8 devices in a mesh: batch: 1 (over z), row: 2 (over y), col: 4 (over x, core).
Axes of the slice: x: 2, y: 2, z: 1, core: 2. Of those that a mesh axis runs over, the one named last changes fastest.
Arguments:
- spd_blocks: float32 [64, 128, 8192], P(('batch', 'row'), None, 'col')
Outputs:
- output: float32 [64, 128, 8192], P(('batch', 'row'), None, 'col')
All inputs are finite; a program needn't handle non-finite values.
Results may differ from the reference program's by a relative error of at most 0.001.
Values are sent between devices in bfloat16 or wider.
A program may use at most 1 GiB of HBM per device.

```python
import math
import jax
import jax.numpy as jnp
from jax import lax

BLOCK = 128
ORDER = 8192
ROW_DEVS = 2
COL_DEVS = 4

BLOCK_COUNT = ORDER // BLOCK


def to_logical(a_cyc):
    by_rows = a_cyc.reshape(ROW_DEVS, BLOCK_COUNT // ROW_DEVS, BLOCK, ORDER).transpose(1, 0, 2, 3)
    by_cols = by_rows.reshape(ORDER, COL_DEVS, BLOCK_COUNT // COL_DEVS, BLOCK).transpose(0, 2, 1, 3)
    return by_cols.reshape(ORDER, ORDER)


def to_cyclic(matrix):
    by_rows = matrix.reshape(BLOCK_COUNT // ROW_DEVS, ROW_DEVS, BLOCK, ORDER).transpose(1, 0, 2, 3)
    by_cols = by_rows.reshape(ORDER, BLOCK_COUNT // COL_DEVS, COL_DEVS, BLOCK).transpose(0, 2, 1, 3)
    return by_cols.reshape(BLOCK_COUNT, BLOCK, ORDER)


def setup_inputs(seed: int = 0, part: int = 0) -> dict:
    rng_key = jax.random.fold_in(jax.random.key(seed), part)
    gauss_draw = jax.random.normal(rng_key, (ORDER, ORDER), jnp.float32)
    sym_part = (gauss_draw + gauss_draw.T) * math.sqrt(0.5 / ORDER)
    matrix = (sym_part + 2.2 * jnp.eye(ORDER, dtype=jnp.float32)) * ORDER
    return {"spd_blocks": to_cyclic(matrix)}


def reference(spd_blocks):
    trailing = to_logical(spd_blocks)
    columns = []
    for step_idx in range(BLOCK_COUNT):
        diag_fac = jnp.tril(jnp.linalg.cholesky(trailing[:BLOCK, :BLOCK]))
        pieces = [jnp.zeros((step_idx * BLOCK, BLOCK), jnp.float32), diag_fac]
        if step_idx + 1 < BLOCK_COUNT:
            panel_f32 = lax.linalg.triangular_solve(diag_fac, trailing[BLOCK:, :BLOCK], left_side=False, lower=True, transpose_a=True)
            pieces.append(panel_f32)
            panel_b16 = panel_f32.astype(jnp.bfloat16)
            trailing = trailing[BLOCK:, BLOCK:] - jnp.dot(panel_b16, panel_b16.T, preferred_element_type=jnp.float32)
        columns.append(jnp.concatenate(pieces, axis=0))
    return to_cyclic(jnp.concatenate(columns, axis=1))
```

```python
import jax
import jax.numpy as jnp
from jax import lax
from jax.experimental import pallas as pl
from jax.experimental.pallas import tpu as pltpu
from jax.sharding import PartitionSpec as P

NB = 64
BS = 128
ROWB = 32
COLB = 16
CHB = 4
NCH = ROWB // CHB
F32 = jnp.float32
BF16 = jnp.bfloat16
HI = lax.Precision.HIGHEST


def dot_nt(a, b, precision=None):
    return lax.dot_general(a, b, (((1,), (1,)), ((), ())), precision=precision, preferred_element_type=F32)


def factor_block(src_ref, g_ref):
    g_ref[...] = src_ref[...]
    for sb in range(4):
        lo = 32 * sb
        part = g_ref[lo:lo + 32, :]
        done_rows = []
        for tb in range(4):
            base = lo + 8 * tb
            rows = part.shape[0]
            lane = lax.broadcasted_iota(jnp.int32, (rows, BS), 1)
            row = lax.broadcasted_iota(jnp.int32, (rows, BS), 0)
            lane8 = lane[0:8]
            row8 = row[0:8]
            cols = [jnp.broadcast_to(part[:, base + q:base + q + 1], (rows, BS)) for q in range(8)]
            scale = jnp.zeros((8, BS), F32)
            for i in range(8):
                piv = jnp.broadcast_to(cols[i][i:i + 1, :], (8, BS))
                rs = lax.rsqrt(piv)
                inv = rs * rs
                scale = jnp.where(row8 == i, rs, scale)
                prow = jnp.broadcast_to(part[i:i + 1, :], (8, BS))
                nrow = jnp.where(lane8 == base + i, inv, prow * inv)
                mult = [jnp.where(row8 > i, cols[i][0:8], 0.0)] + [cols[i][8 * v:8 * v + 8] for v in range(1, rows // 8)]
                hit = [(lane8 == base + i) & (row8 > i)] + [lane8 == base + i] * (rows // 8 - 1)
                part = jnp.concatenate(
                    [jnp.where(hit[v], 0.0, part[8 * v:8 * v + 8]) - mult[v] * nrow for v in range(rows // 8)], axis=0)
                for q in range(i + 1, 8):
                    cq = cols[q]
                    t = jnp.broadcast_to(cq[i:i + 1, :], (8, BS)) * inv
                    cols[q] = jnp.concatenate(
                        [cq[8 * v:8 * v + 8] - mult[v] * t for v in range(rows // 8)], axis=0)
            done_rows.append(jnp.where(lane8 == row8 + base, 1.0, part[0:8]) * scale)
            if tb < 3:
                part = part[8:]
        panel = jnp.concatenate(done_rows, axis=0)
        g_ref[lo:lo + 32, :] = panel
        if sb < 3:
            lane = lax.broadcasted_iota(jnp.int32, (32, BS), 1)
            row = lax.broadcasted_iota(jnp.int32, (32, BS), 0)
            clean = jnp.where((lane < lo + 32) & (lane > row + lo), 0.0, panel)
            upd = lax.dot_general(panel, clean, (((0,), (0,)), ((), ())), precision=HI, preferred_element_type=F32)
            lane = lax.broadcasted_iota(jnp.int32, (96 - lo, BS), 1)
            keep = (lane < lo) | (lane >= lo + 32)
            g_ref[lo + 32:, :] = jnp.where(keep, g_ref[lo + 32:, :], 0.0) - upd[lo + 32:, :]


def kernel(a_hbm, o_hbm, mat, pan, g_ref, ch_d, ch_e, ch_f, ch_r, b1, b2, b1p, b2p,
           in_s, in_b, linv_in, stage,
           ld_sem, out_sem, rrow, rcol, s_src, s_fwd, in_s_sem, in_b_sem, st_sem, bst_sem,
           l_recv, l_send, done, init_recv, init_send):
    r = lax.axis_index("row")
    c = lax.axis_index("col")
    is_chain = (r == 0) & (c == 0)
    xc = c // 2

    bar = pltpu.get_barrier_semaphore()
    for rr in range(2):
        for cc in range(4):
            @pl.when((r != rr) | (c != cc))
            def _(rr=rr, cc=cc):
                pl.semaphore_signal(bar, inc=1, device_id={"row": rr, "col": cc}, device_id_type=pl.DeviceIdType.MESH)
    pl.semaphore_wait(bar, 7)

    def remote(src, dst, ssem, rsem, rr, cc):
        return pltpu.make_async_remote_copy(src_ref=src, dst_ref=dst, send_sem=ssem, recv_sem=rsem,
                                            device_id={"row": rr, "col": cc},
                                            device_id_type=pl.DeviceIdType.MESH)

    def load_col(s):
        return pltpu.make_async_copy(a_hbm.at[:, :, pl.ds(s * BS, BS)], mat.at[s], ld_sem.at[s])

    def out_col(s):
        off = pl.multiple_of(s * BS, BS)
        return pltpu.make_async_copy(mat.at[s], o_hbm.at[:, :, pl.ds(off, BS)], out_sem.at[s])

    for s in range(COLB):
        load_col(s).start()
    pan[2] = jnp.zeros(pan.shape[1:], BF16)
    for s in range(COLB):
        load_col(s).wait()

    init = [((0, 0), ch_d, None), ((1, 0), ch_e, None), ((1, 1), ch_f, None),
            ((2, 0), ch_r, 0), ((2, 1), ch_r, 1), ((2, 2), ch_r, 2)]
    for n, ((bi, bj), buf, sub) in enumerate(init):
        dst = buf if sub is None else buf.at[sub]
        own = (bi % 2, bj % 4)
        src = mat.at[bj // 4, bi // 2]
        if own == (0, 0):
            @pl.when(is_chain)
            def _(dst=dst, src=src):
                dst[...] = src[...]
        else:
            cp = remote(src, dst, init_send.at[n], init_recv.at[n], 0, 0)

            @pl.when((r == own[0]) & (c == own[1]))
            def _(cp=cp):
                cp.start()
                cp.wait_send()

            @pl.when(is_chain)
            def _(cp=cp):
                cp.wait_recv()

    def first_chunk(k, par):
        return ((k + 2 - par) // 2) // CHB

    def col_block(buf, s):
        idx = jnp.where(r == c % 2, 2 * s + xc, ROWB + s)
        return pan[buf, idx // 2, idx % 2]

    def row_copy(buf, q, ssem, rr, cc):
        return remote(pan.at[buf, pl.ds(2 * q, 2)], pan.at[buf, pl.ds(2 * q, 2)], ssem, rrow.at[buf, q], rr, cc)

    def col_copy(buf, q, half, ssem, rr, cc):
        return remote(pan.at[buf, pl.ds(2 * q, 2), half], pan.at[buf, COLB + q], ssem, rcol.at[buf, q], rr, cc)

    def step(k, carry):
        buf = lax.rem(k, 3)
        pbuf = lax.rem(k + 2, 3)
        ck = lax.rem(k, 4)
        cp_ = lax.rem(k + 3, 4)
        slot4 = lax.rem(k, 4)
        pslot4 = lax.rem(k + 3, 4)
        lslot = lax.rem(k // 4, 2)
        own_col = c == ck
        sk = k // 4

        def linv_copy(par):
            return remote(g_ref, linv_in.at[lslot], l_send.at[par], l_recv.at[lslot], par, ck)

        @pl.when(is_chain)
        def _():
            factor_block(ch_d, g_ref)

            @pl.when(ck == 0)
            def _():
                linv_in[lslot] = g_ref[...]

            @pl.when(ck != 0)
            def _():
                linv_copy(0).start()
            linv_copy(1).start()

            @pl.when(k < NB - 1)
            def _():
                lane = lax.broadcasted_iota(jnp.int32, (BS, BS), 1)
                row = lax.broadcasted_iota(jnp.int32, (BS, BS), 0)
                linv = jnp.where(lane <= row, g_ref[...], 0.0)
                x1 = dot_nt(ch_e[...], linv, HI).astype(BF16)
                b1[...] = x1
                ch_d[...] = ch_f[...] - dot_nt(x1, x1)

        pk = k - 1
        src_prev = c == cp_
        fwd_prev = (c % 2 == 1) & (xc != cp_ // 2) & (k > 0)
        q_row = first_chunk(pk, r)
        q_col = first_chunk(pk, 1 - r)

        @pl.when(k > 0)
        def _():
            def take(q, _):
                @pl.when(jnp.logical_not(src_prev))
                def _():
                    row_copy(pbuf, q, s_fwd.at[0, q], r, c).wait_recv()

                @pl.when(fwd_prev)
                def _():
                    row_copy(pbuf, q, s_fwd.at[0, q], r, c - 1).start()
                    col_copy(pbuf, q, xc, s_fwd.at[1, q], 1 - r, 2 * xc + r).start()
                return 0
            lax.fori_loop(q_row, NCH, take, 0)

            @pl.when(r != c % 2)
            def _():
                def take_col(q, _):
                    col_copy(pbuf, q, xc, s_fwd.at[1, q], 1 - r, c).wait_recv()
                    return 0
                lax.fori_loop(q_col, NCH, take_col, 0)

        row3 = k + 3
        t3 = row3 // 2
        b_copy = remote(pan.at[buf, t3 // 2, t3 % 2], in_b.at[slot4], bst_sem, in_b_sem.at[slot4], 0, 0)
        send_b = own_col & (row3 < NB) & (r == row3 % 2)

        @pl.when(own_col)
        def _():
            @pl.when(jnp.logical_not(is_chain))
            def _():
                linv_copy(r).wait_recv()

            @pl.when(k >= 3)
            def _():
                pl.semaphore_wait(done.at[lslot], 7)
            q0 = first_chunk(k, r)
            t0 = (k + 2 - r) // 2

            def clear(q, _):
                mat[sk, pl.ds(CHB * q, CHB)] = jnp.zeros((CHB, BS, BS), F32)
                return 0
            lax.fori_loop(0, q0, clear, 0)

            lane = lax.broadcasted_iota(jnp.int32, (BS, BS), 1)
            row = lax.broadcasted_iota(jnp.int32, (BS, BS), 0)

            def solve(q, _):
                linv = jnp.where(lane <= row, linv_in[lslot], 0.0)
                left = pan[pbuf, pl.ds(2 * q, 2)].reshape(CHB * BS, BS)
                cur = mat[sk, pl.ds(CHB * q, CHB)].reshape(CHB * BS, BS) - dot_nt(left, col_block(pbuf, sk))
                x = dot_nt(cur, linv, HI)
                rowid = lax.broadcasted_iota(jnp.int32, (CHB * BS, BS), 0)
                x = jnp.where(rowid >= (t0 - CHB * q) * BS, x, 0.0)
                mat[sk, pl.ds(CHB * q, CHB)] = x.reshape(CHB, BS, BS)
                pan[buf, pl.ds(2 * q, 2)] = x.astype(BF16).reshape(2, 2, BS, BS)
                row_copy(buf, q, s_src.at[0, q], r, 2 * xc + (1 - c % 2)).start()
                row_copy(buf, q, s_src.at[1, q], r, 2 * (1 - xc) + 1).start()
                col_copy(buf, q, xc, s_src.at[2, q], 1 - r, 2 * xc + r).start()

                @pl.when(send_b & (q == t3 // CHB))
                def _():
                    @pl.when(is_chain)
                    def _():
                        in_b[slot4] = pan[buf, t3 // 2, t3 % 2]

                    @pl.when(jnp.logical_not(is_chain))
                    def _():
                        b_copy.start()
                return 0
            lax.fori_loop(q0, NCH, solve, 0)

            @pl.when(r == k % 2)
            def _():
                g = linv_in[lslot]
                up = jnp.where(lane > row, g, jnp.where(lane == row, 1.0 / g, 0.0))
                mat[sk, k // 2] = up.T
            out_col(sk).start()

        m = lax.rem(c - k + 64, 4)
        send_s = (row3 < NB) & (r == row3 % 2) & (m != 0)
        msl = jnp.maximum(m - 1, 0)
        s_copy = remote(stage, in_s.at[slot4, msl], st_sem, in_s_sem.at[slot4, msl], 0, 0)

        @pl.when(send_s)
        def _():
            sm = (k + m) // 4
            val = mat[sm, t3] - dot_nt(pan[pbuf, t3 // 2, t3 % 2], col_block(pbuf, sm))

            @pl.when(is_chain)
            def _():
                in_s[slot4, msl] = val

            @pl.when(jnp.logical_not(is_chain))
            def _():
                stage[...] = val
                s_copy.start()

        @pl.when(k > 0)
        def _():
            s_lo = (k - c + 4) // 4

            def chunk(q, cols_, right):
                left = pan[pbuf, pl.ds(2 * q, 2)].reshape(CHB * BS, BS)
                u = dot_nt(left, right)
                for n, s in enumerate(cols_):
                    un = u[:, n * BS:(n + 1) * BS].reshape(CHB, BS, BS)
                    mat[s, pl.ds(CHB * q, CHB)] = mat[s, pl.ds(CHB * q, CHB)] - un

            def low_chunk(s):
                return ((4 * s + c - r + 1) // 2) // CHB

            @pl.when((s_lo % 2 == 1) & (s_lo < COLB))
            def _():
                def body(q, _):
                    chunk(q, (s_lo,), col_block(pbuf, s_lo))
                    return 0
                lax.fori_loop(low_chunk(s_lo), NCH, body, 0)

            def pair(sp, _):
                s0 = 2 * sp

                def body(q, _):
                    right = jnp.concatenate([col_block(pbuf, s0), col_block(pbuf, s0 + 1)], axis=0)
                    chunk(q, (s0, s0 + 1), right)
                    return 0
                lax.fori_loop(low_chunk(s0), NCH, body, 0)
                return 0
            lax.fori_loop((s_lo + 1) // 2, COLB // 2, pair, 0)

        @pl.when(send_s & jnp.logical_not(is_chain))
        def _():
            s_copy.wait_send()

        @pl.when(send_b & jnp.logical_not(is_chain))
        def _():
            b_copy.wait_send()

        @pl.when(k > 0)
        def _():
            def drain(q, _):
                @pl.when(src_prev)
                def _():
                    row_copy(pbuf, q, s_src.at[0, q], r, c).wait_send()
                    row_copy(pbuf, q, s_src.at[1, q], r, c).wait_send()
                    col_copy(pbuf, q, xc, s_src.at[2, q], r, c).wait_send()

                @pl.when(fwd_prev)
                def _():
                    row_copy(pbuf, q, s_fwd.at[0, q], r, c).wait_send()
                    col_copy(pbuf, q, xc, s_fwd.at[1, q], r, c).wait_send()
                return 0
            lax.fori_loop(q_row, NCH, drain, 0)

        @pl.when((k >= 1) & (k + 2 < NB))
        def _():
            tc = lax.rem(k + 2, 4)
            nslot = lax.rem((k + 2) // 4, 2)
            for rr in range(2):
                @pl.when((r != rr) | (c != tc))
                def _(rr=rr):
                    pl.semaphore_signal(done.at[nslot], inc=1, device_id={"row": rr, "col": tc},
                                        device_id_type=pl.DeviceIdType.MESH)

        @pl.when(is_chain)
        def _():
            @pl.when((k > 0) & (k + 2 < NB))
            def _():
                rown = k + 2
                for mm in range(3):
                    ocol = lax.rem(k + mm, 4)

                    @pl.when((rown % 2 != 0) | (ocol != 0))
                    def _(mm=mm):
                        remote(stage, in_s.at[pslot4, mm], st_sem, in_s_sem.at[pslot4, mm], 0, 0).wait_recv()

                @pl.when((rown % 2 != 0) | (cp_ != 0))
                def _():
                    remote(in_b.at[pslot4], in_b.at[pslot4], bst_sem, in_b_sem.at[pslot4], 0, 0).wait_recv()
                bn = in_b[pslot4]
                ch_r[0] = in_s[pslot4, 0] - dot_nt(bn, b1p[...])
                ch_r[1] = in_s[pslot4, 1] - dot_nt(bn, b2p[...])
                ch_r[2] = in_s[pslot4, 2] - dot_nt(bn, bn)

            @pl.when(k + 2 < NB)
            def _():
                lane = lax.broadcasted_iota(jnp.int32, (BS, BS), 1)
                row = lax.broadcasted_iota(jnp.int32, (BS, BS), 0)
                linv = jnp.where(lane <= row, g_ref[...], 0.0)
                x2 = dot_nt(ch_r[0], linv, HI).astype(BF16)
                b2[...] = x2
                ch_e[...] = ch_r[1] - dot_nt(x2, b1[...])
                ch_f[...] = ch_r[2] - dot_nt(x2, x2)
                b1p[...] = b1[...]
                b2p[...] = x2

            @pl.when(ck != 0)
            def _():
                linv_copy(0).wait_send()
            linv_copy(1).wait_send()
        return carry

    lax.fori_loop(0, NB, step, 0)
    for s in range(COLB):
        out_col(s).wait()


def solution(mesh):
    blk = lambda *shape: pltpu.VMEM(shape + (BS, BS), F32)
    bb = lambda *shape: pltpu.VMEM(shape + (BS, BS), BF16)
    dma = pltpu.SemaphoreType.DMA
    call = pl.pallas_call(
        kernel,
        out_shape=jax.ShapeDtypeStruct((ROWB, BS, COLB * BS), F32),
        in_specs=[pl.BlockSpec(memory_space=pl.ANY)],
        out_specs=pl.BlockSpec(memory_space=pl.ANY),
        scratch_shapes=[
            blk(COLB, ROWB), bb(3, 24, 2), blk(), blk(), blk(), blk(), blk(3), bb(), bb(), bb(), bb(),
            blk(4, 3), bb(4), blk(2), blk(),
            dma((COLB,)), dma((COLB,)), dma((3, NCH)), dma((3, NCH)), dma((3, NCH)), dma((2, NCH)),
            dma((4, 3)), dma((4,)), dma(()), dma(()),
            dma((2,)), dma((2,)), pltpu.SemaphoreType.REGULAR((2,)), dma((6,)), dma((6,)),
        ],
        compiler_params=pltpu.CompilerParams(collective_id=0, has_side_effects=True, vmem_limit_bytes=60 * 1024 * 1024),
        name="chol",
    )
    spec = P(("batch", "row"), None, "col")
    return jax.shard_map(lambda a: call(a), mesh=mesh, in_specs=(spec,), out_specs=spec, check_vma=False)
```

```python
import jax
import jax.numpy as jnp
from jax import lax
from jax.experimental import pallas as pl
from jax.experimental.pallas import tpu as pltpu
from jax.sharding import PartitionSpec as P

NB = 64
BS = 128
ROWB = 32
COLB = 16
CHB = 2
NCH = ROWB // CHB
DCB = 4
NBUF = 5
F32 = jnp.float32
BF16 = jnp.bfloat16
HI = lax.Precision.HIGHEST


def dot_nt(a, b, precision=None):
    return lax.dot_general(a, b, (((1,), (1,)), ((), ())), precision=precision, preferred_element_type=F32)


def factor_block(src_ref, g_ref):
    g_ref[...] = src_ref[...]
    for sb in range(4):
        lo = 32 * sb
        part = g_ref[lo:lo + 32, :]
        done_rows = []
        for tb in range(4):
            base = lo + 8 * tb
            rows = part.shape[0]
            lane = lax.broadcasted_iota(jnp.int32, (rows, BS), 1)
            row = lax.broadcasted_iota(jnp.int32, (rows, BS), 0)
            lane8 = lane[0:8]
            row8 = row[0:8]
            cols = [jnp.broadcast_to(part[:, base + q:base + q + 1], (rows, BS)) for q in range(8)]
            scale = jnp.zeros((8, BS), F32)
            for i in range(8):
                piv = jnp.broadcast_to(cols[i][i:i + 1, :], (8, BS))
                rs = lax.rsqrt(piv)
                inv = rs * rs
                scale = jnp.where(row8 == i, rs, scale)
                prow = jnp.broadcast_to(part[i:i + 1, :], (8, BS))
                nrow = jnp.where(lane8 == base + i, inv, prow * inv)
                mult = [jnp.where(row8 > i, cols[i][0:8], 0.0)] + [cols[i][8 * v:8 * v + 8] for v in range(1, rows // 8)]
                hit = [(lane8 == base + i) & (row8 > i)] + [lane8 == base + i] * (rows // 8 - 1)
                part = jnp.concatenate(
                    [jnp.where(hit[v], 0.0, part[8 * v:8 * v + 8]) - mult[v] * nrow for v in range(rows // 8)], axis=0)
                for q in range(i + 1, 8):
                    cq = cols[q]
                    t = jnp.broadcast_to(cq[i:i + 1, :], (8, BS)) * inv
                    cols[q] = jnp.concatenate(
                        [cq[8 * v:8 * v + 8] - mult[v] * t for v in range(rows // 8)], axis=0)
            done_rows.append(jnp.where(lane8 == row8 + base, 1.0, part[0:8]) * scale)
            if tb < 3:
                part = part[8:]
        panel = jnp.concatenate(done_rows, axis=0)
        g_ref[lo:lo + 32, :] = panel
        if sb < 3:
            lane = lax.broadcasted_iota(jnp.int32, (32, BS), 1)
            row = lax.broadcasted_iota(jnp.int32, (32, BS), 0)
            clean = jnp.where((lane < lo + 32) & (lane > row + lo), 0.0, panel)
            upd = lax.dot_general(panel, clean, (((0,), (0,)), ((), ())), precision=HI, preferred_element_type=F32)
            lane = lax.broadcasted_iota(jnp.int32, (96 - lo, BS), 1)
            keep = (lane < lo) | (lane >= lo + 32)
            g_ref[lo + 32:, :] = jnp.where(keep, g_ref[lo + 32:, :], 0.0) - upd[lo + 32:, :]


def kernel(a_hbm, o_hbm, mat, pan, g_ref, ch_d, ch_e, ch_f, ch_r, b1, b2, b1p, b2p,
           in_s, in_b, linv_in, stage,
           ld_sem, out_sem, rrow, rcol, s_src, s_fwd, in_s_sem, in_b_sem, st_sem, bst_sem,
           l_recv, l_send, done, init_recv, init_send):
    r = lax.axis_index("row")
    c = lax.axis_index("col")
    is_chain = (r == 0) & (c == 0)
    xc = c // 2

    bar = pltpu.get_barrier_semaphore()
    for rr in range(2):
        for cc in range(4):
            @pl.when((r != rr) | (c != cc))
            def _(rr=rr, cc=cc):
                pl.semaphore_signal(bar, inc=1, device_id={"row": rr, "col": cc}, device_id_type=pl.DeviceIdType.MESH)
    pl.semaphore_wait(bar, 7)

    def remote(src, dst, ssem, rsem, rr, cc):
        return pltpu.make_async_remote_copy(src_ref=src, dst_ref=dst, send_sem=ssem, recv_sem=rsem,
                                            device_id={"row": rr, "col": cc},
                                            device_id_type=pl.DeviceIdType.MESH)

    def load_col(s):
        return pltpu.make_async_copy(a_hbm.at[:, :, pl.ds(s * BS, BS)], mat.at[s], ld_sem.at[s])

    def out_col(s):
        off = pl.multiple_of(s * BS, BS)
        return pltpu.make_async_copy(mat.at[s], o_hbm.at[:, :, pl.ds(off, BS)], out_sem.at[s])

    for s in range(COLB):
        load_col(s).start()
    pan[NBUF - 1] = jnp.zeros(pan.shape[1:], BF16)
    pan[NBUF - 2] = jnp.zeros(pan.shape[1:], BF16)
    for s in range(COLB):
        load_col(s).wait()

    init = [((0, 0), ch_d, None), ((1, 0), ch_e, None), ((1, 1), ch_f, None),
            ((2, 0), ch_r, 0), ((2, 1), ch_r, 1), ((2, 2), ch_r, 2)]
    for n, ((bi, bj), buf, sub) in enumerate(init):
        dst = buf if sub is None else buf.at[sub]
        own = (bi % 2, bj % 4)
        src = mat.at[bj // 4, bi // 2]
        if own == (0, 0):
            @pl.when(is_chain)
            def _(dst=dst, src=src):
                dst[...] = src[...]
        else:
            cp = remote(src, dst, init_send.at[n], init_recv.at[n], 0, 0)

            @pl.when((r == own[0]) & (c == own[1]))
            def _(cp=cp):
                cp.start()
                cp.wait_send()

            @pl.when(is_chain)
            def _(cp=cp):
                cp.wait_recv()

    def first_chunk(k, par):
        return ((k + 2 - par) // 2) // CHB

    def col_block(buf, s):
        idx = jnp.where(r == c % 2, 2 * s + xc, ROWB + s)
        return pan[buf, idx // 2, idx % 2]

    def row_copy(buf, q, ssem, rr, cc):
        return remote(pan.at[buf, q], pan.at[buf, q], ssem, rrow.at[buf, q], rr, cc)

    def col_copy(buf, q, half, ssem, rr, cc):
        return remote(pan.at[buf, q, half], pan.at[buf, COLB + q // 2, q % 2], ssem, rcol.at[buf, q], rr, cc)

    def drain_panel(p):
        b = lax.rem(p, NBUF)
        cs = lax.rem(p, 4)

        def body(q, _):
            @pl.when(c == cs)
            def _():
                row_copy(b, q, s_src.at[b, 0, q], r, c).wait_send()
                row_copy(b, q, s_src.at[b, 1, q], r, c).wait_send()
                col_copy(b, q, xc, s_src.at[b, 2, q], r, c).wait_send()

                @pl.when(q < first_chunk(p, r) + 2)
                def _():
                    row_copy(b, q, s_src.at[b, 3, q], r, c).wait_send()
                    col_copy(b, q, xc, s_src.at[b, 4, q], r, c).wait_send()

            @pl.when((c % 2 == 1) & (xc != cs // 2) & (q >= first_chunk(p, r) + 2))
            def _():
                row_copy(b, q, s_fwd.at[b, 0, q], r, c).wait_send()
                col_copy(b, q, xc, s_fwd.at[b, 1, q], r, c).wait_send()
            return 0
        lax.fori_loop(first_chunk(p, r), NCH, body, 0)

    def step(k, carry):
        buf = lax.rem(k, NBUF)
        pbuf = lax.rem(k + NBUF - 1, NBUF)
        obuf = lax.rem(k + NBUF - 2, NBUF)
        ck = lax.rem(k, 4)
        cp_ = lax.rem(k + 3, 4)
        slot4 = lax.rem(k, 4)
        pslot4 = lax.rem(k + 3, 4)
        lslot = lax.rem(k // 4, 2)
        own_col = c == ck
        sk = k // 4

        def linv_copy(par):
            return remote(g_ref, linv_in.at[lslot], l_send.at[par], l_recv.at[lslot], par, ck)

        @pl.when(is_chain)
        def _():
            factor_block(ch_d, g_ref)

            @pl.when(ck == 0)
            def _():
                linv_in[lslot] = g_ref[...]

            @pl.when(ck != 0)
            def _():
                linv_copy(0).start()
            linv_copy(1).start()

            @pl.when(k < NB - 1)
            def _():
                lane = lax.broadcasted_iota(jnp.int32, (BS, BS), 1)
                row = lax.broadcasted_iota(jnp.int32, (BS, BS), 0)
                linv = jnp.where(lane <= row, g_ref[...], 0.0)
                x1 = dot_nt(ch_e[...], linv, HI).astype(BF16)
                b1[...] = x1
                ch_d[...] = ch_f[...] - dot_nt(x1, x1)

        pk = k - 1
        src_prev = c == cp_
        fwd_prev = (c % 2 == 1) & (xc != cp_ // 2) & (k > 0)
        q_row = first_chunk(pk, r)
        q_col = first_chunk(pk, 1 - r)
        q_row2 = jnp.minimum(q_row + 2, NCH)
        q_col2 = jnp.minimum(q_col + 2, NCH)

        c2 = lax.rem(k + 2, 4)
        late = (k > 1) & (c != c2) & (c != cp_) & jnp.logical_not((c % 2 == 1) & (xc != c2 // 2))
        q_late = jnp.minimum(first_chunk(k - 2, r) + 2, NCH)

        def take_late(q):
            row_copy(obuf, q, s_fwd.at[obuf, 0, q], r, c).wait_recv()

        def take_row(q):
            @pl.when(jnp.logical_not(src_prev) & (k > 0))
            def _():
                row_copy(pbuf, q, s_fwd.at[pbuf, 0, q], r, c).wait_recv()

            @pl.when(fwd_prev & (q >= q_row + 2))
            def _():
                row_copy(pbuf, q, s_fwd.at[pbuf, 0, q], r, c - 1).start()
                col_copy(pbuf, q, xc, s_fwd.at[pbuf, 1, q], 1 - r, 2 * xc + r).start()

        def take_rows(lo, hi):
            def body(q, _):
                take_row(q)
                return 0
            lax.fori_loop(lo, hi, body, 0)

        def take_cols(b, lo, hi):
            @pl.when(r != c % 2)
            def _():
                def body(q, _):
                    col_copy(b, q, xc, s_fwd.at[b, 1, q], 1 - r, c).wait_recv()
                    return 0
                lax.fori_loop(lo, hi, body, 0)

        @pl.when(k > 0)
        def _():
            take_cols(pbuf, q_col, jnp.minimum(q_col + 1, NCH))
            take_rows(q_row, jnp.where(own_col, jnp.minimum(q_row + 1, NCH), q_row2))

        row3 = k + 3
        t3 = row3 // 2
        b_copy = remote(pan.at[buf, t3 // 2, t3 % 2], in_b.at[slot4], bst_sem, in_b_sem.at[slot4], 0, 0)
        send_b = own_col & (row3 < NB) & (r == row3 % 2)

        @pl.when(own_col)
        def _():
            @pl.when(jnp.logical_not(is_chain))
            def _():
                linv_copy(r).wait_recv()

            @pl.when(k >= NBUF - 2)
            def _():
                pl.semaphore_wait(done.at[lslot], 7)
            q0 = first_chunk(k, r)
            t0 = (k + 2 - r) // 2

            def clear(q, _):
                mat[sk, pl.ds(CHB * q, CHB)] = jnp.zeros((CHB, BS, BS), F32)
                return 0
            lax.fori_loop(0, q0, clear, 0)

            lane = lax.broadcasted_iota(jnp.int32, (BS, BS), 1)
            row = lax.broadcasted_iota(jnp.int32, (BS, BS), 0)

            def solve(q, _):
                linv = jnp.where(lane <= row, linv_in[lslot], 0.0)
                @pl.when((q > q_row) & (k > 0))
                def _():
                    take_row(q)

                @pl.when(late & (q >= q_late))
                def _():
                    take_late(q)
                left = jnp.concatenate([pan[obuf, q].reshape(CHB * BS, BS),
                                        pan[pbuf, q].reshape(CHB * BS, BS)], axis=1)
                right = jnp.concatenate([col_block(obuf, sk), col_block(pbuf, sk)], axis=1)
                cur = mat[sk, pl.ds(CHB * q, CHB)].reshape(CHB * BS, BS) - dot_nt(left, right)
                x = dot_nt(cur, linv, HI)
                rowid = lax.broadcasted_iota(jnp.int32, (CHB * BS, BS), 0)
                x = jnp.where(rowid >= (t0 - CHB * q) * BS, x, 0.0)
                mat[sk, pl.ds(CHB * q, CHB)] = x.reshape(CHB, BS, BS)
                pan[buf, q] = x.astype(BF16).reshape(CHB, BS, BS)
                @pl.when(send_b & (q == t3 // CHB))
                def _():
                    @pl.when(is_chain)
                    def _():
                        in_b[slot4] = pan[buf, t3 // 2, t3 % 2]

                    @pl.when(jnp.logical_not(is_chain))
                    def _():
                        b_copy.start()

                row_copy(buf, q, s_src.at[buf, 0, q], r, 2 * xc + (1 - c % 2)).start()
                row_copy(buf, q, s_src.at[buf, 1, q], r, 2 * (1 - xc) + 1).start()
                col_copy(buf, q, xc, s_src.at[buf, 2, q], 1 - r, 2 * xc + r).start()

                @pl.when(q < q0 + 2)
                def _():
                    row_copy(buf, q, s_src.at[buf, 3, q], r, 2 * (1 - xc)).start()
                    col_copy(buf, q, 1 - xc, s_src.at[buf, 4, q], 1 - r, 2 * (1 - xc) + r).start()
                return 0
            lax.fori_loop(q0, NCH, solve, 0)

            @pl.when(r == k % 2)
            def _():
                g = linv_in[lslot]
                up = jnp.where(lane > row, g, jnp.where(lane == row, 1.0 / g, 0.0))
                mat[sk, k // 2] = up.T
            out_col(sk).start()

        @pl.when(k > 0)
        def _():
            take_cols(pbuf, jnp.minimum(q_col + 1, NCH), q_col2)

        m = lax.rem(c - k + 64, 4)
        send_s = (row3 < NB) & (r == row3 % 2) & (m != 0)
        msl = jnp.maximum(m - 1, 0)
        s_copy = remote(stage, in_s.at[slot4, msl], st_sem, in_s_sem.at[slot4, msl], 0, 0)

        @pl.when(send_s)
        def _():
            sm = (k + m) // 4
            left = jnp.concatenate([pan[obuf, t3 // 2, t3 % 2], pan[pbuf, t3 // 2, t3 % 2]], axis=1)
            right = jnp.concatenate([col_block(obuf, sm), col_block(pbuf, sm)], axis=1)
            val = mat[sm, t3] - dot_nt(left, right)

            @pl.when(is_chain)
            def _():
                in_s[slot4, msl] = val

            @pl.when(jnp.logical_not(is_chain))
            def _():
                stage[...] = val
                s_copy.start()

        @pl.when(fwd_prev & jnp.logical_not(own_col))
        def _():
            take_rows(q_row2, NCH)

        @pl.when(k > 1)
        def _():
            take_cols(obuf, jnp.minimum(first_chunk(k - 2, 1 - r) + 2, NCH), NCH)

            @pl.when(late & jnp.logical_not(own_col))
            def _():
                def body(q, _):
                    take_late(q)
                    return 0
                lax.fori_loop(q_late, NCH, body, 0)

        @pl.when(k > 1)
        def _():
            s_lo = (k - c + 4) // 4

            def chunk(q, cols_, right):
                left = pan[obuf, pl.ds(2 * q, 2)].reshape(DCB * BS, BS)
                u = dot_nt(left, right)
                for n, s in enumerate(cols_):
                    un = u[:, n * BS:(n + 1) * BS].reshape(DCB, BS, BS)
                    mat[s, pl.ds(DCB * q, DCB)] = mat[s, pl.ds(DCB * q, DCB)] - un

            def low_chunk(s):
                return ((4 * s + c - r + 1) // 2) // DCB

            @pl.when((s_lo % 2 == 1) & (s_lo < COLB))
            def _():
                def body(q, _):
                    chunk(q, (s_lo,), col_block(obuf, s_lo))
                    return 0
                lax.fori_loop(low_chunk(s_lo), ROWB // DCB, body, 0)

            def pair(sp, _):
                s0 = 2 * sp

                def body(q, _):
                    right = jnp.concatenate([col_block(obuf, s0), col_block(obuf, s0 + 1)], axis=0)
                    chunk(q, (s0, s0 + 1), right)
                    return 0
                lax.fori_loop(low_chunk(s0), ROWB // DCB, body, 0)
                return 0
            lax.fori_loop((s_lo + 1) // 2, COLB // 2, pair, 0)

        @pl.when(send_s & jnp.logical_not(is_chain))
        def _():
            s_copy.wait_send()

        @pl.when(send_b & jnp.logical_not(is_chain))
        def _():
            b_copy.wait_send()

        @pl.when(k > 1)
        def _():
            drain_panel(k - 2)

        @pl.when(k - 2 + NBUF < NB)
        def _():
            tc = lax.rem(k - 2 + NBUF, 4)
            nslot = lax.rem((k - 2 + NBUF) // 4, 2)
            for rr in range(2):
                @pl.when((r != rr) | (c != tc))
                def _(rr=rr):
                    pl.semaphore_signal(done.at[nslot], inc=1, device_id={"row": rr, "col": tc},
                                        device_id_type=pl.DeviceIdType.MESH)

        @pl.when(is_chain)
        def _():
            @pl.when((k > 0) & (k + 2 < NB))
            def _():
                rown = k + 2
                for mm in range(3):
                    ocol = lax.rem(k + mm, 4)

                    @pl.when((rown % 2 != 0) | (ocol != 0))
                    def _(mm=mm):
                        remote(stage, in_s.at[pslot4, mm], st_sem, in_s_sem.at[pslot4, mm], 0, 0).wait_recv()

                @pl.when((rown % 2 != 0) | (cp_ != 0))
                def _():
                    remote(in_b.at[pslot4], in_b.at[pslot4], bst_sem, in_b_sem.at[pslot4], 0, 0).wait_recv()
                bn = in_b[pslot4]
                ch_r[0] = in_s[pslot4, 0] - dot_nt(bn, b1p[...])
                ch_r[1] = in_s[pslot4, 1] - dot_nt(bn, b2p[...])
                ch_r[2] = in_s[pslot4, 2] - dot_nt(bn, bn)

            @pl.when(k + 2 < NB)
            def _():
                lane = lax.broadcasted_iota(jnp.int32, (BS, BS), 1)
                row = lax.broadcasted_iota(jnp.int32, (BS, BS), 0)
                linv = jnp.where(lane <= row, g_ref[...], 0.0)
                x2 = dot_nt(ch_r[0], linv, HI).astype(BF16)
                b2[...] = x2
                ch_e[...] = ch_r[1] - dot_nt(x2, b1[...])
                ch_f[...] = ch_r[2] - dot_nt(x2, x2)
                b1p[...] = b1[...]
                b2p[...] = x2

            @pl.when(ck != 0)
            def _():
                linv_copy(0).wait_send()
            linv_copy(1).wait_send()
        return carry

    lax.fori_loop(0, NB, step, 0)
    drain_panel(jnp.int32(NB - 2))
    for s in range(COLB):
        out_col(s).wait()


def solution(mesh):
    blk = lambda *shape: pltpu.VMEM(shape + (BS, BS), F32)
    bb = lambda *shape: pltpu.VMEM(shape + (BS, BS), BF16)
    dma = pltpu.SemaphoreType.DMA
    call = pl.pallas_call(
        kernel,
        out_shape=jax.ShapeDtypeStruct((ROWB, BS, COLB * BS), F32),
        in_specs=[pl.BlockSpec(memory_space=pl.ANY)],
        out_specs=pl.BlockSpec(memory_space=pl.ANY),
        scratch_shapes=[
            blk(COLB, ROWB), bb(NBUF, 24, 2), blk(), blk(), blk(), blk(), blk(3), bb(), bb(), bb(), bb(),
            blk(4, 3), bb(4), blk(2), blk(),
            dma((COLB,)), dma((COLB,)), dma((NBUF, NCH)), dma((NBUF, NCH)), dma((NBUF, 5, NCH)), dma((NBUF, 2, NCH)),
            dma((4, 3)), dma((4,)), dma(()), dma(()),
            dma((2,)), dma((2,)), pltpu.SemaphoreType.REGULAR((2,)), dma((6,)), dma((6,)),
        ],
        compiler_params=pltpu.CompilerParams(collective_id=0, has_side_effects=True, vmem_limit_bytes=60 * 1024 * 1024),
        name="chol",
    )
    spec = P(("batch", "row"), None, "col")
    return jax.shard_map(lambda a: call(a), mesh=mesh, in_specs=(spec,), out_specs=spec, check_vma=False)
```
